32 devices in a mesh: tm: 16 (over z, x, core), space: 2 (over y).
Axes of the slice: x: 2, y: 2, z: 4, core: 2. Of those that a mesh axis runs over, the one named last changes fastest.
Arguments:
- forcing: float32 [16, 8, 128, 128], P('tm', 'space'), may hold values from -6 to 6
- initial: float32 [8, 128, 128], P('space'), may hold values from -6 to 6
- coupling: float32 [8, 128, 128], P('space'), may hold values from 0.3 to 3
- velocity: float32 [3, 8, 128, 128], P(None, 'space'), may hold values from -0.9 to 0.9
Outputs:
- iterate: float32 [16, 8, 128, 128], P('tm', 'space')
The draws below stay inside these ranges and needn't reach their ends.
All inputs are finite; a program needn't handle non-finite values.
Results may differ from the reference program's by a relative error of at most 0.0003.
Values sent between devices are 32-bit elements; how exact they have to be, the bound alone decides.
A program may use at most 64 MiB of HBM per device.

```python
import math
import jax
import jax.numpy as jnp
from jax import lax

NY = 128
NX = 128
ITERS = 2
SWEEPS = 8
NT = 16
NZ = 8


def level_of(stream_key, shape, cuts, low, top_value):
    level = 1.0
    for axis_at, parts in cuts:
        draws = jax.random.uniform(jax.random.fold_in(jax.random.fold_in(stream_key, 6), axis_at), (parts,), jnp.float32, low / len(cuts), top_value / len(cuts))
        level = level * jnp.repeat(jnp.exp(draws), shape[axis_at] // parts).reshape((-1,) + (1,) * (len(shape) - 1 - axis_at))
    return level


def gaussian(key, dims, width, reach, shards=(), kind=jnp.bfloat16):
    array = width * jax.random.normal(key, dims, jnp.float32)
    if shards:
        array = array * level_of(key, dims, shards, -0.22, 0.18)
    return jnp.clip(array, -reach, reach).astype(kind)


def setup_inputs(seed: int = 0) -> dict:
    arg_keys = jax.random.split(jax.random.key(seed), 5)
    forcing = gaussian(arg_keys[0], (NT, NZ, NY, NX), 1.0, 6.0, ((0, 16), (1, 2)), jnp.float32)
    initial = gaussian(arg_keys[1], (NZ, NY, NX), 1.0, 6.0, ((0, 2),), jnp.float32)
    coupling = jnp.clip(jnp.exp(math.log(3.0) - 2.3025851 * jax.random.uniform(arg_keys[2], (NZ, NY, NX), jnp.float32) ** level_of(arg_keys[2], (NZ, NY, NX), ((0, 2),), -0.2, 0.2)), 0.3, 3.0)
    velocity = jnp.clip(jax.random.uniform(arg_keys[3], (3, NZ, NY, NX), jnp.float32, -0.9, 0.9) * level_of(arg_keys[3], (3, NZ, NY, NX), ((1, 2),), -0.4, 0.0), -0.9, 0.9)
    return dict(forcing=forcing, initial=initial, coupling=coupling, velocity=velocity)


wrap_alpha = 0.1


def padded(field):
    widths = [(0, 0)] * (field.ndim - 3) + [(1, 1)] * 3
    return jnp.pad(field, widths)


def coupled(extended, coupling, advect):
    total = (coupling - advect[0]) * extended[..., 2:, 1:-1, 1:-1] + (coupling + advect[0]) * extended[..., :-2, 1:-1, 1:-1]
    total = total + (coupling - advect[1]) * extended[..., 1:-1, 2:, 1:-1] + (coupling + advect[1]) * extended[..., 1:-1, :-2, 1:-1]
    total = total + (coupling - advect[2]) * extended[..., 1:-1, 1:-1, 2:] + (coupling + advect[2]) * extended[..., 1:-1, 1:-1, :-2]
    return total


def tables(total_steps):
    indices = jnp.arange(total_steps, dtype=jnp.int32)
    products = (indices[:, None] * indices[None, :]) % total_steps
    angles = products.astype(jnp.float32) * (2.0 * math.pi / total_steps)
    return jnp.cos(angles), jnp.sin(angles)


def matmul(table, columns):
    return jnp.dot(table, columns, preferred_element_type=jnp.float32, precision=lax.Precision.HIGHEST)


def reference(forcing, initial, coupling, velocity):
    total_steps = forcing.shape[0]
    shape = forcing.shape
    advect = coupling[None] * velocity
    cosine, sine_table = tables(total_steps)
    steps_float = jnp.arange(total_steps, dtype=jnp.float32)
    time_weight = jnp.exp(math.log(wrap_alpha) * steps_float / total_steps)[:, None, None, None]
    radius = math.exp(math.log(wrap_alpha) / total_steps)
    angles = steps_float * (2.0 * math.pi / total_steps)
    shift_re = radius * jnp.cos(angles)
    shift_im = radius * jnp.sin(angles)
    iterate = jnp.broadcast_to(initial, shape).astype(jnp.float32)

    def solve(pieces):
        source_re, source_im, freq_re, freq_im = pieces
        diag_re = 1.0 + 6.0 * coupling - freq_re
        diag_im = freq_im
        modulus = diag_re * diag_re + diag_im * diag_im
        value_re = (source_re * diag_re + source_im * diag_im) / modulus
        value_im = (source_im * diag_re - source_re * diag_im) / modulus
        for sweep in range(SWEEPS):
            sum_re = source_re + coupled(padded(value_re), coupling, advect)
            sum_im = source_im + coupled(padded(value_im), coupling, advect)
            value_re = (sum_re * diag_re + sum_im * diag_im) / modulus
            value_im = (sum_im * diag_re - sum_re * diag_im) / modulus
        return value_re, value_im

    for repeat in range(ITERS):
        previous = jnp.concatenate([initial[None], iterate[:-1]], axis=0)
        residual = forcing - ((1.0 + 6.0 * coupling) * iterate - coupled(padded(iterate), coupling, advect)) + previous
        columns = (residual * time_weight).reshape(total_steps, -1)
        spec_re = matmul(cosine, columns).reshape(shape)
        spec_im = (-matmul(sine_table, columns)).reshape(shape)
        value_re, value_im = lax.map(solve, (spec_re, spec_im, shift_re, shift_im))
        inverse_part = (matmul(cosine, value_re.reshape(total_steps, -1)) - matmul(sine_table, value_im.reshape(total_steps, -1))) / total_steps
        iterate = iterate + inverse_part.reshape(shape) / time_weight
    return iterate
```

```python
import math

import jax
import jax.numpy as jnp
import numpy as np
from jax import lax
from jax.experimental import pallas as pl
from jax.experimental.pallas import tpu as pltpu
from jax.sharding import PartitionSpec as P

ITERS = 2
SWEEPS = 8
HALO = 8
GUARD = SWEEPS + 1

wrap_alpha = 0.1


def by_index(index, values):
    picked = jnp.float32(values[0])
    for at in range(1, len(values)):
        picked = jnp.where(index == at, jnp.float32(values[at]), picked)
    return picked


def weighted(terms):
    total = None
    for weight, value in terms:
        if abs(weight) < 1e-12:
            continue
        if abs(weight - 1.0) < 1e-12:
            term = value
        elif abs(weight + 1.0) < 1e-12:
            term = None
            total = -value if total is None else total - value
        else:
            term = value * float(weight)
        if term is not None:
            total = term if total is None else total + term
    return total


def plus(first, second):
    return second if first is None else first if second is None else first + second


def minus(first, second):
    return first if second is None else -second if first is None else first - second


def forward_transform(values):
    T = len(values)
    U = T // 2
    gamma = [wrap_alpha ** (n / T) for n in range(T)]
    a = [values[n] if n == 0 else values[n] * float(gamma[n]) for n in range(T)]
    even = {n: a[n] + a[T - n] for n in range(1, U)}
    odd = {n: a[n] - a[T - n] for n in range(1, U)}

    def cosine(u, parity):
        return weighted([(math.cos(2 * math.pi * u * n / T), even[n]) for n in range(1, U) if n % 2 == parity])

    def sine(u, parity):
        return weighted([(math.sin(2 * math.pi * u * n / T), odd[n]) for n in range(1, U) if n % 2 == parity])

    result = [None] * U
    ends = [a[0] + a[U], a[0] - a[U]]
    zero_even = plus(ends[0], cosine(0, 0))
    zero_odd = cosine(0, 1)
    result[0] = (plus(zero_even, zero_odd), minus(zero_even, zero_odd))
    for u in range(1, U // 2 + 1):
        c_even = plus(ends[u % 2], cosine(u, 0))
        c_odd = cosine(u, 1)
        s_even, s_odd = sine(u, 0), sine(u, 1)
        if u == U - u:
            result[u] = (plus(c_even, c_odd), minus(None, plus(s_even, s_odd)))
            continue
        result[u] = (plus(c_even, c_odd), minus(None, plus(s_even, s_odd)))
        result[U - u] = (minus(c_even, c_odd), minus(s_even, s_odd))
    return result


def inverse_transform(pairs, begin):
    U = len(pairs)
    T = 2 * U
    scale = [1.0 / (T * wrap_alpha ** (m / T)) for m in range(T)]
    first, middle = pairs[0]
    ends = [first + middle, first - middle]

    def cosine(m, parity):
        return weighted([(2 * math.cos(2 * math.pi * u * m / T), pairs[u][0]) for u in range(1, U) if u % 2 == parity])

    def sine(m, parity):
        return weighted([(2 * math.sin(2 * math.pi * u * m / T), pairs[u][1]) for u in range(1, U) if u % 2 == parity])

    result = [None] * T

    def put(m, real, imaginary):
        for at, value in ((m, minus(real, imaginary)), ((T - m) % T, plus(real, imaginary))):
            if result[at] is None:
                result[at] = begin + value * float(scale[at])

    for m in range(0, U // 2 + 1):
        c_even, c_odd = plus(ends[m % 2], cosine(m, 0)), cosine(m, 1)
        s_even, s_odd = sine(m, 0), sine(m, 1)
        put(m, plus(c_even, c_odd), plus(s_even, s_odd))
        other = U - m
        if other != m:
            put(other, minus(c_even, c_odd), minus(s_odd, s_even))
    return result


def kernel(
    dims,
    f_hbm,
    i_hbm,
    c_hbm,
    v_hbm,
    out_ref,
    fbuf,
    ini,
    kc,
    times,
    fields,
    edge,
    kin,
    coef,
    pq,
    land,
    src,
    wa,
    wb,
    wc,
    part,
    gathered,
    reduced,
    last,
    fin,
    back,
    states,
    sl,
    s1,
    r1,
    s2,
    r2,
    sk,
    rk,
    sf,
    rf,
    se,
    re,
    sw,
    rw,
    ss,
    rs,
    sg,
    rg,
    s3,
    r3,
    s4,
    r4,
):
    T, S, NY, NX, zl = dims
    U = T // 2
    NZ = zl * S
    C = zl * NY // T
    bands = 2 * S
    R = NY // bands
    RH = R + 2 * HALO
    WC = C + 2 * HALO
    q = C // R
    PK = RH + 3 * HALO
    PS = RH + HALO
    PF = R + HALO
    chunk_rows = R * NZ // U
    edges = HALO * U // R
    rho = wrap_alpha ** (1.0 / T)
    O = GUARD

    t = lax.axis_index("tm")
    s = lax.axis_index("space")
    group = t // zl
    zi = t % zl
    at = zi * S + s
    unit = at // q
    band = group * q + at % q
    plane = s * zl + zi
    row0 = pl.multiple_of(group * C, 8)

    def place(u, b):
        spot = u * q + b % q
        return (b // q) * zl + spot // S, spot % S

    def chunk(tt):
        start = (tt % zl) * NY + (tt // zl) * C
        return pl.ds(pl.multiple_of(start, 8), C)

    def device(tt, ts):
        return {"tm": tt, "space": ts}

    def remote(source, target, ssem, rsem, tt, ts):
        return pltpu.make_async_remote_copy(
            src_ref=source,
            dst_ref=target,
            send_sem=ssem,
            recv_sem=rsem,
            device_id=device(tt, ts),
            device_id_type=pl.DeviceIdType.MESH,
        )

    barrier = pltpu.get_barrier_semaphore()
    for m in range(T - 1, 0, -1):
        pl.semaphore_signal(barrier, inc=1, device_id=device(t ^ m, s), device_id_type=pl.DeviceIdType.MESH)
    for m in range(1, S):
        pl.semaphore_signal(barrier, inc=1, device_id=device(t, s ^ m), device_id_type=pl.DeviceIdType.MESH)

    def window(start, count):
        first = jnp.clip(start - HALO, 0, NY - count)
        offset = HALO + first - (start - HALO)
        return pl.ds(pl.multiple_of(first, 8), count), pl.ds(pl.multiple_of(offset, 8), count)

    def space_window(ts):
        return window((group * q + (zi * S + ts) % q) * R, RH)

    own = pl.ds(s * zl, zl)
    k_from, k_to = space_window(s)
    i_from, i_to = window(row0, WC)
    local = [
        pltpu.make_async_copy(f_hbm, fbuf, sl.at[0]),
        pltpu.make_async_copy(i_hbm.at[:, i_from], ini.at[:, i_to], sl.at[1]),
        pltpu.make_async_copy(c_hbm.at[zi, pl.ds(row0, C)], kc.at[0], sl.at[2]),
        pltpu.make_async_copy(v_hbm.at[:, zi, pl.ds(row0, C)], kc.at[pl.ds(1, 3)], sl.at[3]),
        pltpu.make_async_copy(c_hbm.at[:, k_from], kin.at[0, own, k_to], sl.at[4]),
        pltpu.make_async_copy(v_hbm.at[:, :, k_from], kin.at[pl.ds(1, 3), own, k_to], sl.at[5]),
    ]
    for copy in local:
        copy.start()

    @pl.when(group == 0)
    def _():
        ini[:, HALO : 2 * HALO] = jnp.zeros((zl, HALO, NX), jnp.float32)

    @pl.when(row0 + C == NY)
    def _():
        ini[:, WC : WC + HALO] = jnp.zeros((zl, HALO, NX), jnp.float32)

    @pl.when(band == 0)
    def _():
        kin[:, :, HALO : 2 * HALO] = jnp.zeros((4, NZ, HALO, NX), jnp.float32)

    @pl.when(band == bands - 1)
    def _():
        kin[:, :, RH : RH + HALO] = jnp.zeros((4, NZ, HALO, NX), jnp.float32)

    pl.semaphore_wait(barrier, T + S - 2)
    sent = []

    def send(source, target, ssem, rsem, tt, ts, valid=None, maybe_self=False):
        copy = remote(source, target, ssem, rsem, tt, ts)
        away = valid
        if maybe_self:
            same = jnp.logical_and(tt == t, ts == s)
            here = same if valid is None else jnp.logical_and(valid, same)
            away = jnp.logical_not(same)
            if valid is not None:
                away = jnp.logical_and(valid, away)

            @pl.when(here)
            def _():
                pltpu.make_async_copy(source, target, rsem).start()

        if away is None:
            copy.start()
            sent.append(copy.wait_send)
        else:

            @pl.when(away)
            def _():
                copy.start()

            def finish():
                @pl.when(away)
                def _():
                    copy.wait_send()

            sent.append(finish)

    def arrived(target, rsem, valid=None):
        if valid is None:
            pltpu.make_async_copy(target, target, rsem).wait()
        else:

            @pl.when(valid)
            def _():
                pltpu.make_async_copy(target, target, rsem).wait()

    local[0].wait()
    for m in range(T - 1, 0, -1):
        tt = t ^ m
        send(fbuf.at[chunk(tt)], times.at[t], s1.at[m], r1.at[m], tt, s)
    inner_rows = pl.ds(row0, C)
    up_s = jnp.minimum(s + 1, S - 1)
    down_s = jnp.maximum(s - 1, 0)
    send(i_hbm.at[zl - 1, inner_rows], edge.at[0], se.at[0], re.at[0], t, up_s, valid=s + 1 < S)
    send(i_hbm.at[0, inner_rows], edge.at[1], se.at[1], re.at[1], t, down_s, valid=s > 0)
    half = zl // 2
    share = (t % 2) * half
    rest = half - share
    partner = t ^ 1
    for m in range(1, S):
        ts = s ^ m
        from_rows, to_rows = space_window(ts)
        give = pl.ds(share, half)
        put = pl.ds(s * zl + share, half)
        send(c_hbm.at[give, from_rows], kin.at[0, put, to_rows], sk.at[m, 0], rk.at[m, 0], t, ts)
        send(v_hbm.at[:, give, from_rows], kin.at[pl.ds(1, 3), put, to_rows], sk.at[m, 1], rk.at[m, 1], t, ts)
    times[pl.ds(t, 1)] = fbuf[chunk(t)][None]
    for copy in local[1:]:
        copy.wait()

    def shifted(value, by, axis):
        return pltpu.roll(value, by % value.shape[axis], axis)

    column = lax.broadcasted_iota(jnp.int32, (C, NX), 1)
    arrived(edge.at[0], re.at[0], valid=s > 0)
    arrived(edge.at[1], re.at[1], valid=s + 1 < S)

    @pl.when(s == 0)
    def _():
        edge[0] = jnp.zeros((C, NX), jnp.float32)

    @pl.when(s + 1 == S)
    def _():
        edge[1] = jnp.zeros((C, NX), jnp.float32)

    inner = pl.ds(2 * HALO, C)
    wide = ini[zi, pl.ds(HALO, WC)]
    middle = wide[HALO : HALO + C]
    lower = jnp.where(zi == 0, edge[0], ini[jnp.maximum(zi - 1, 0), inner])
    upper = jnp.where(zi == zl - 1, edge[1], ini[jnp.minimum(zi + 1, zl - 1), inner])
    coupling = kc[0]
    adz = coupling * kc[1]
    ady = coupling * kc[2]
    adx = coupling * kc[3]
    summed = (coupling - adz) * upper + (coupling + adz) * lower
    summed += (coupling - ady) * shifted(wide, -1, 0)[HALO : HALO + C]
    summed += (coupling + ady) * shifted(wide, 1, 0)[HALO : HALO + C]
    summed += (coupling - adx) * jnp.where(column == NX - 1, 0.0, shifted(middle, -1, 1))
    summed += (coupling + adx) * jnp.where(column == 0, 0.0, shifted(middle, 1, 1))
    start = summed - 6.0 * coupling * middle

    for m in range(1, T):
        arrived(times.at[t ^ m], r1.at[m])

    for block in range(C // 8):
        rows = slice(block * 8, block * 8 + 8)
        spectrum = forward_transform([times[m, rows] + start[rows] for m in range(T)])
        for u in range(U):
            for p in range(2):
                fields[u, p, rows] = spectrum[u][p]

    kinds = ((0, R, HALO), (0, HALO, HALO + R), (R - HALO, HALO, 0))

    def lying(z, first, count):
        return land.at[:, pl.ds(pl.multiple_of(z * PS + first, 8), count)]

    for m in range(NZ - 1, -1, -1):
        spot = at ^ m
        u = spot // q
        o = spot % q
        b = group * q + o
        for kind in range(3):
            to = b + (0, -1, 1)[kind]
            valid = (None, to >= 0, to < bands)[kind]
            first, count, put = kinds[kind]
            source = fields.at[u, :, pl.ds(pl.multiple_of(o * R + first, 8), count)]
            if kind == 0 and m == 0:
                own_rows = pl.ds(pl.multiple_of(plane * PS + put, 8), count)
                land[:, own_rows] = fields[u, :, pl.ds(pl.multiple_of(o * R, 8), R)]
                continue
            to_t, to_s = place(u, jnp.clip(to, 0, bands - 1))
            send(
                source,
                lying(plane, put, count),
                s2.at[m, kind],
                r2.at[plane, kind],
                to_t,
                to_s,
                valid=valid,
                maybe_self=kind > 0 and q > 1,
            )

    for m in range(1, S):
        theirs = (s ^ m) * zl
        block_c = kin.at[0, pl.ds(theirs + share, half), k_to]
        block_v = kin.at[pl.ds(1, 3), pl.ds(theirs + share, half), k_to]
        arrived(block_c, rk.at[m, 0])
        arrived(block_v, rk.at[m, 1])
        send(block_c, block_c, sf.at[m, 0], rf.at[m, 0], partner, s)
        send(block_v, block_v, sf.at[m, 1], rf.at[m, 1], partner, s)
    for m in range(1, S):
        theirs = (s ^ m) * zl
        arrived(kin.at[0, pl.ds(theirs + rest, half), k_to], rf.at[m, 0])
        arrived(kin.at[pl.ds(1, 3), pl.ds(theirs + rest, half), k_to], rf.at[m, 1])

    angles = [2.0 * math.pi * u / U / 2 for u in range(U)]
    shift_re1 = by_index(unit, [rho * math.cos(a) for a in angles])
    shift_im1 = by_index(unit, [0.0] + [rho * math.sin(a) for a in angles[1:]])
    shift_re2 = by_index(unit, [-rho] + [rho * math.cos(a) for a in angles[1:]])
    z_at = lax.broadcasted_iota(jnp.int32, (NZ, NX), 0)
    x_at = lax.broadcasted_iota(jnp.int32, (NZ, NX), 1)

    def line(y):
        if isinstance(y, int):
            return pl.ds((y + O) * NZ, NZ)
        return pl.ds(pl.multiple_of((y + O) * NZ, 8), NZ)

    flat_kin = kin.reshape(4, NZ * PK, NX)

    @pl.loop(0, RH, unroll=4)
    def _(i):
        c, vz, vy, vx = [flat_kin[m, pl.ds(i + HALO, NZ, stride=PK)] for m in range(4)]
        to = line(i - HALO)
        az = c * vz
        ay = c * vy
        ax = c * vx
        zero = jnp.zeros_like(c)
        coef[0, to] = jnp.where(z_at == NZ - 1, zero, c - az)
        coef[1, to] = jnp.where(z_at == 0, zero, c + az)
        coef[2, to] = c - ay
        coef[3, to] = c + ay
        coef[4, to] = jnp.where(x_at == NX - 1, zero, c - ax)
        coef[5, to] = jnp.where(x_at == 0, zero, c + ax)
        diag1 = 1.0 + 6.0 * c - shift_re1
        diag2 = 1.0 + 6.0 * c - shift_re2
        im2 = shift_im1 * shift_im1
        modulus1 = diag1 * diag1 + im2
        modulus2 = diag2 * diag2 + im2
        pq[0, to] = diag1 / modulus1
        pq[1, to] = diag2 / modulus2
        pq[2, to] = shift_im1 / modulus1

    @pl.when(band == 0)
    def _():
        for z in range(NZ):
            land[:, z * PS : z * PS + HALO] = jnp.zeros((2, HALO, NX), jnp.float32)
        last[: HALO * NZ] = jnp.zeros((HALO * NZ, NX), jnp.float32)

    @pl.when(band == bands - 1)
    def _():
        for z in range(NZ):
            land[:, z * PS + HALO + R : z * PS + RH] = jnp.zeros((2, HALO, NX), jnp.float32)
        last[(HALO + R) * NZ :] = jnp.zeros((HALO * NZ, NX), jnp.float32)

    reach = -(-GUARD // R)
    counts = [min(R, GUARD - j * R) for j in range(reach)]
    for j in range(reach):
        spread = counts[j] * NZ

        @pl.when(band < j + 1)
        def _(j=j, spread=spread):
            first = (O - j * R - counts[j]) * NZ
            wc[:, first : first + spread] = jnp.zeros((2, spread, NX), jnp.float32)

        @pl.when(band + j + 1 > bands - 1)
        def _(j=j, spread=spread):
            first = (O + R + j * R) * NZ
            wc[:, first : first + spread] = jnp.zeros((2, spread, NX), jnp.float32)

    for m in range(NZ):
        z = plane ^ m
        if m:
            arrived(lying(z, HALO, R), r2.at[z, 0])
        arrived(lying(z, HALO + R, HALO), r2.at[z, 1], valid=band < bands - 1)
        arrived(lying(z, 0, HALO), r2.at[z, 2], valid=band > 0)

    def scaled(y, re_part, im_part):
        p1, p2, im = pq[0, line(y)], pq[1, line(y)], pq[2, line(y)]
        return re_part * p1 + im_part * im, im_part * p2 - re_part * im

    def neighbours(old, y, p):
        here = old[p, line(y)]
        total = src[p, line(y)] + coef[2, line(y)] * old[p, line(y + 1)] + coef[3, line(y)] * old[p, line(y - 1)]
        total += coef[0, line(y)] * shifted(here, -1, 0) + coef[1, line(y)] * shifted(here, 1, 0)
        total += coef[4, line(y)] * shifted(here, -1, 1) + coef[5, line(y)] * shifted(here, 1, 1)
        return total

    def sweep(old, new, low, high):
        for y in range(low, high):
            re_part, im_part = scaled(y, neighbours(old, y, 0), neighbours(old, y, 1))
            new[0, line(y)] = re_part
            new[1, line(y)] = im_part

    for y in range(-HALO, R + HALO):
        pair = [land[p, pl.ds(y + HALO, NZ, stride=PS)] for p in range(2)]
        src[0, line(y)] = pair[0]
        src[1, line(y)] = pair[1]
        re_part, im_part = scaled(y, *pair)
        wa[0, line(y)] = re_part
        wa[1, line(y)] = im_part
    old, new = wa, wb
    for k in range(1, SWEEPS):
        sweep(old, new, k - HALO, R + HALO - k)
        old, new = new, old
    weight = [2.0 * math.cos(2.0 * math.pi * u * (T - 1) / T) / T for u in range(U)]
    weight[0] = 1.0 / T
    other = [-2.0 * math.sin(2.0 * math.pi * u * (T - 1) / T) / T for u in range(U)]
    other[0] = (1.0 - 2.0 * ((T - 1) % 2)) / T
    weight_re = by_index(unit, [rho * w for w in weight])
    weight_im = by_index(unit, [rho * w for w in other])
    for y in range(R):
        re_part, im_part = scaled(y, neighbours(old, y, 0), neighbours(old, y, 1))
        wc[0, line(y)] = re_part
        wc[1, line(y)] = im_part
        part[y * NZ : y * NZ + NZ] = weight_re * re_part + weight_im * im_part

    def piece(u):
        return pl.ds(pl.multiple_of(u * chunk_rows, 8), chunk_rows)

    for m in range(U - 1, 0, -1):
        u = unit ^ m
        send(part.at[piece(u)], gathered.at[m], ss.at[m], rs.at[m], *place(u, band))

    def span(first, count):
        return pl.ds((first + O) * NZ, count * NZ)

    for j in range(reach):
        count = counts[j]
        above = jnp.minimum(band + j + 1, bands - 1)
        below = jnp.maximum(band - j - 1, 0)
        to_above = wc.at[:, span(-j * R - count, count)]
        to_below = wc.at[:, span(R + j * R, count)]
        source = wc.at[:, span(R - count, count)]
        send(source, to_above, sw.at[j, 0], rw.at[j, 0], *place(unit, above), valid=band + j + 1 < bands)
        source = wc.at[:, span(0, count)]
        send(source, to_below, sw.at[j, 1], rw.at[j, 1], *place(unit, below), valid=band >= j + 1)
    earlier = list(sent)
    sent.clear()
    for m in range(1, U):
        arrived(gathered.at[m], rs.at[m])
    total = part[piece(unit)]
    for m in range(1, U):
        total = total + gathered[m]
    reduced[...] = total
    base = HALO * NZ
    mine = pl.ds(pl.multiple_of(base + unit * chunk_rows, 8), chunk_rows)
    last[mine] = total
    low_at = pl.ds(pl.multiple_of((HALO + R) * NZ + jnp.minimum(unit, edges - 1) * chunk_rows, 8), chunk_rows)
    high_at = pl.ds(pl.multiple_of(jnp.maximum(unit - (U - edges), 0) * chunk_rows, 8), chunk_rows)
    goes_down = jnp.logical_and(band > 0, unit < edges)
    goes_up = jnp.logical_and(band < bands - 1, unit >= U - edges)
    for m in range(U - 1, -1, -1):
        u = unit ^ m
        below = place(u, jnp.maximum(band - 1, 0))
        above = place(u, jnp.minimum(band + 1, bands - 1))
        send(reduced, last.at[low_at], sg.at[m, 1], rg.at[m, 1], *below, valid=goes_down)
        send(reduced, last.at[high_at], sg.at[m, 2], rg.at[m, 2], *above, valid=goes_up)
        if m:
            send(reduced, last.at[mine], sg.at[m, 0], rg.at[m, 0], *place(u, band))
    for j in range(reach):
        count = counts[j]
        arrived(wc.at[:, span(-j * R - count, count)], rw.at[j, 0], valid=band >= j + 1)
        arrived(wc.at[:, span(R + j * R, count)], rw.at[j, 1], valid=band + j + 1 < bands)
    for y in range(-HALO, R + HALO):
        wa[0, line(y)] = neighbours(wc, y, 0)
        wa[1, line(y)] = neighbours(wc, y, 1)
    for finish in earlier:
        finish()
    for m in range(U):
        u = unit ^ m
        if m:
            arrived(last.at[pl.ds(pl.multiple_of(base + u * chunk_rows, 8), chunk_rows)], rg.at[m, 0])
        here = pl.ds(pl.multiple_of((HALO + R) * NZ + jnp.minimum(u, edges - 1) * chunk_rows, 8), chunk_rows)
        arrived(last.at[here], rg.at[m, 1], valid=jnp.logical_and(band < bands - 1, u < edges))
        here = pl.ds(pl.multiple_of(jnp.maximum(u - (U - edges), 0) * chunk_rows, 8), chunk_rows)
        arrived(last.at[here], rg.at[m, 2], valid=jnp.logical_and(band > 0, u >= U - edges))

    both = jnp.where(unit == 0, jnp.float32(1.0), jnp.float32(0.0))
    for y in range(-HALO, R + HALO):
        wrap = last[(y + HALO) * NZ : (y + HALO + 1) * NZ]
        wrap_im = wrap * both
        src[0, line(y)] = src[0, line(y)] - wrap
        src[1, line(y)] = src[1, line(y)] - wrap_im
        re_part, im_part = scaled(y, wa[0, line(y)] - wrap, wa[1, line(y)] - wrap_im)
        wb[0, line(y)] = re_part
        wb[1, line(y)] = im_part
    old, new = wb, wa
    for k in range(2, SWEEPS + 1):
        sweep(old, new, k - GUARD, R + GUARD - k)
        old, new = new, old
    for y in range(R):
        re_part, im_part = scaled(y, neighbours(old, y, 0), neighbours(old, y, 1))
        fin[0, pl.ds(y, NZ, stride=PF)] = re_part
        fin[1, pl.ds(y, NZ, stride=PF)] = im_part

    offset = pl.multiple_of((band % q) * R, 8)
    for m in range(NZ - 1, -1, -1):
        z = plane ^ m
        source = pl.ds(pl.multiple_of(z * PF, 8), R)
        if m == 0:
            back[pl.ds(unit, 1), :, pl.ds(offset, R)] = fin[:, source][None]
            continue
        send(
            fin.at[:, source],
            back.at[unit, :, pl.ds(offset, R)],
            s3.at[m],
            r3.at[unit, band % q],
            group * zl + z % zl,
            z // zl,
        )
    for m in range(1, U * q):
        spot = at ^ m
        u = spot // q
        o = spot % q
        arrived(back.at[u, :, pl.ds(pl.multiple_of(o * R, 8), R)], r3.at[u, o])
    for block in range(C // 8):
        rows = slice(block * 8, block * 8 + 8)
        result = inverse_transform([(back[u, 0, rows], back[u, 1, rows]) for u in range(U)], middle[rows])
        for m in range(T):
            states[m, rows] = result[m]
    for m in range(T - 1, 0, -1):
        tt = t ^ m
        send(states.at[tt], out_ref.at[chunk(t)], s4.at[m], r4.at[m], tt, s)
    out_ref[chunk(t)] = states[pl.ds(t, 1)][0]
    for finish in sent:
        finish()
    for m in range(1, T):
        arrived(out_ref.at[chunk(t ^ m)], r4.at[m])


def body(forcing, initial, coupling, velocity):
    local_steps, zl, NY, NX = forcing.shape
    T = lax.axis_size("tm")
    S = lax.axis_size("space")
    U = T // 2
    NZ = zl * S
    C = zl * NY // T
    bands = 2 * S
    R = NY // bands
    RH = R + 2 * HALO
    WC = C + 2 * HALO
    q = C // R
    PK = RH + 3 * HALO
    PS = RH + HALO
    PF = R + HALO
    rows = R + 2 * GUARD
    reach = -(-GUARD // R)
    assert local_steps == 1 and SWEEPS == HALO <= R and ITERS == 2
    assert S % q == 0 and zl % 2 == 0 and T % 4 == 0
    assert C % R == 0 and NY % C == 0 and U * q == NZ and NZ % 8 == 0
    assert T & (T - 1) == 0 and S & (S - 1) == 0 and NZ & (NZ - 1) == 0
    assert (R * NZ // U) % 8 == 0 and (HALO * U) % R == 0 and WC <= NY
    f32 = jnp.float32
    dma = pltpu.SemaphoreType.DMA
    hbm = pl.BlockSpec(memory_space=pltpu.HBM)
    out = pl.pallas_call(
        lambda *refs: kernel((T, S, NY, NX, zl), *refs),
        out_shape=jax.ShapeDtypeStruct((zl * NY, NX), f32),
        in_specs=[hbm] * 4,
        out_specs=pl.BlockSpec(memory_space=pltpu.VMEM),
        scratch_shapes=[
            pltpu.VMEM((zl * NY, NX), f32),
            pltpu.VMEM((zl, WC + 2 * HALO, NX), f32),
            pltpu.VMEM((4, C, NX), f32),
            pltpu.VMEM((T, C, NX), f32),
            pltpu.VMEM((U, 2, C, NX), f32),
            pltpu.VMEM((2, C, NX), f32),
            pltpu.VMEM((4, NZ, PK, NX), f32),
            pltpu.VMEM((6, rows * NZ, NX), f32),
            pltpu.VMEM((3, rows * NZ, NX), f32),
            pltpu.VMEM((2, NZ * PS, NX), f32),
            pltpu.VMEM((2, rows * NZ, NX), f32),
            pltpu.VMEM((2, rows * NZ, NX), f32),
            pltpu.VMEM((2, rows * NZ, NX), f32),
            pltpu.VMEM((2, rows * NZ, NX), f32),
            pltpu.VMEM((R * NZ, NX), f32),
            pltpu.VMEM((U, R * NZ // U, NX), f32),
            pltpu.VMEM((R * NZ // U, NX), f32),
            pltpu.VMEM((RH * NZ, NX), f32),
            pltpu.VMEM((2, NZ * PF, NX), f32),
            pltpu.VMEM((U, 2, C, NX), f32),
            pltpu.VMEM((T, C, NX), f32),
            dma((6,)),
            dma((T,)),
            dma((T,)),
            dma((NZ, 3)),
            dma((NZ, 3)),
            dma((S, 2)),
            dma((S, 2)),
            dma((S, 2)),
            dma((S, 2)),
            dma((2,)),
            dma((2,)),
            dma((reach, 2)),
            dma((reach, 2)),
            dma((U,)),
            dma((U,)),
            dma((U, 3)),
            dma((U, 3)),
            dma((NZ,)),
            dma((U, q)),
            dma((T,)),
            dma((T,)),
        ],
        compiler_params=pltpu.CompilerParams(
            has_side_effects=True, collective_id=0, vmem_limit_bytes=48 * 1024 * 1024
        ),
    )(forcing.reshape(zl * NY, NX), initial, coupling, velocity)
    return out.reshape(forcing.shape)


def solution(mesh):
    return jax.shard_map(
        body,
        mesh=mesh,
        in_specs=(
            P("tm", "space", None, None),
            P("space", None, None),
            P("space", None, None),
            P(None, "space", None, None),
        ),
        out_specs=P("tm", "space", None, None),
        check_vma=False,
    )
```

```python
import math

import jax
import jax.numpy as jnp
import numpy as np
from jax import lax
from jax.experimental import pallas as pl
from jax.experimental.pallas import tpu as pltpu
from jax.sharding import PartitionSpec as P

ITERS = 2
SWEEPS = 8
HALO = 8
GUARD = SWEEPS + 1

wrap_alpha = 0.1


def by_index(index, values):
    picked = jnp.float32(values[0])
    for at in range(1, len(values)):
        picked = jnp.where(index == at, jnp.float32(values[at]), picked)
    return picked


def weighted(terms):
    total = None
    for weight, value in terms:
        if abs(weight) < 1e-12:
            continue
        if abs(weight - 1.0) < 1e-12:
            term = value
        elif abs(weight + 1.0) < 1e-12:
            term = None
            total = -value if total is None else total - value
        else:
            term = value * float(weight)
        if term is not None:
            total = term if total is None else total + term
    return total


def plus(first, second):
    return second if first is None else first if second is None else first + second


def minus(first, second):
    return first if second is None else -second if first is None else first - second


def forward_transform(values):
    T = len(values)
    U = T // 2
    gamma = [wrap_alpha ** (n / T) for n in range(T)]
    a = [values[n] if n == 0 else values[n] * float(gamma[n]) for n in range(T)]
    even = {n: a[n] + a[T - n] for n in range(1, U)}
    odd = {n: a[n] - a[T - n] for n in range(1, U)}

    def cosine(u, parity):
        return weighted([(math.cos(2 * math.pi * u * n / T), even[n]) for n in range(1, U) if n % 2 == parity])

    def sine(u, parity):
        return weighted([(math.sin(2 * math.pi * u * n / T), odd[n]) for n in range(1, U) if n % 2 == parity])

    result = [None] * U
    ends = [a[0] + a[U], a[0] - a[U]]
    zero_even = plus(ends[0], cosine(0, 0))
    zero_odd = cosine(0, 1)
    result[0] = (plus(zero_even, zero_odd), minus(zero_even, zero_odd))
    for u in range(1, U // 2 + 1):
        c_even = plus(ends[u % 2], cosine(u, 0))
        c_odd = cosine(u, 1)
        s_even, s_odd = sine(u, 0), sine(u, 1)
        if u == U - u:
            result[u] = (plus(c_even, c_odd), minus(None, plus(s_even, s_odd)))
            continue
        result[u] = (plus(c_even, c_odd), minus(None, plus(s_even, s_odd)))
        result[U - u] = (minus(c_even, c_odd), minus(s_even, s_odd))
    return result


def inverse_transform(pairs, begin):
    U = len(pairs)
    T = 2 * U
    scale = [1.0 / (T * wrap_alpha ** (m / T)) for m in range(T)]
    first, middle = pairs[0]
    ends = [first + middle, first - middle]

    def cosine(m, parity):
        return weighted([(2 * math.cos(2 * math.pi * u * m / T), pairs[u][0]) for u in range(1, U) if u % 2 == parity])

    def sine(m, parity):
        return weighted([(2 * math.sin(2 * math.pi * u * m / T), pairs[u][1]) for u in range(1, U) if u % 2 == parity])

    result = [None] * T

    def put(m, real, imaginary):
        for at, value in ((m, minus(real, imaginary)), ((T - m) % T, plus(real, imaginary))):
            if result[at] is None:
                result[at] = begin + value * float(scale[at])

    for m in range(0, U // 2 + 1):
        c_even, c_odd = plus(ends[m % 2], cosine(m, 0)), cosine(m, 1)
        s_even, s_odd = sine(m, 0), sine(m, 1)
        put(m, plus(c_even, c_odd), plus(s_even, s_odd))
        other = U - m
        if other != m:
            put(other, minus(c_even, c_odd), minus(s_odd, s_even))
    return result


def kernel(
    dims,
    f_hbm,
    i_hbm,
    c_hbm,
    v_hbm,
    out_ref,
    fbuf,
    ini,
    kc,
    times,
    fields,
    edge,
    kin,
    coef,
    pq,
    land,
    src,
    wa,
    wb,
    wc,
    part,
    gathered,
    reduced,
    last,
    fin,
    back,
    states,
    sl,
    s1,
    r1,
    s2,
    r2,
    sk,
    rk,
    sf,
    rf,
    se,
    re,
    sw,
    rw,
    ss,
    rs,
    sg,
    rg,
    s3,
    r3,
    s4,
    r4,
):
    T, S, NY, NX, zl = dims
    U = T // 2
    NZ = zl * S
    C = zl * NY // T
    bands = 2 * S
    R = NY // bands
    RH = R + 2 * HALO
    WC = C + 2 * HALO
    q = C // R
    PK = RH + 3 * HALO
    PS = RH + HALO
    PF = R + HALO
    chunk_rows = R * NZ // U
    edges = HALO * U // R
    rho = wrap_alpha ** (1.0 / T)
    O = GUARD

    t = lax.axis_index("tm")
    s = lax.axis_index("space")
    group = t // zl
    zi = t % zl
    at = zi * S + s
    unit = at // q
    band = group * q + at % q
    plane = s * zl + zi
    row0 = pl.multiple_of(group * C, 8)

    def place(u, b):
        spot = u * q + b % q
        return (b // q) * zl + spot // S, spot % S

    def chunk(tt):
        start = (tt % zl) * NY + (tt // zl) * C
        return pl.ds(pl.multiple_of(start, 8), C)

    def device(tt, ts):
        return {"tm": tt, "space": ts}

    def remote(source, target, ssem, rsem, tt, ts):
        return pltpu.make_async_remote_copy(
            src_ref=source,
            dst_ref=target,
            send_sem=ssem,
            recv_sem=rsem,
            device_id=device(tt, ts),
            device_id_type=pl.DeviceIdType.MESH,
        )

    barrier = pltpu.get_barrier_semaphore()
    for m in range(T - 1, 0, -1):
        pl.semaphore_signal(barrier, inc=1, device_id=device(t ^ m, s), device_id_type=pl.DeviceIdType.MESH)
    for m in range(1, S):
        pl.semaphore_signal(barrier, inc=1, device_id=device(t, s ^ m), device_id_type=pl.DeviceIdType.MESH)

    def window(start, count):
        first = jnp.clip(start - HALO, 0, NY - count)
        offset = HALO + first - (start - HALO)
        return pl.ds(pl.multiple_of(first, 8), count), pl.ds(pl.multiple_of(offset, 8), count)

    def space_window(ts):
        return window((group * q + (zi * S + ts) % q) * R, RH)

    own = pl.ds(s * zl, zl)
    k_from, k_to = space_window(s)
    i_from, i_to = window(row0, WC)
    local = [
        pltpu.make_async_copy(f_hbm, fbuf, sl.at[0]),
        pltpu.make_async_copy(i_hbm.at[:, i_from], ini.at[:, i_to], sl.at[1]),
        pltpu.make_async_copy(c_hbm.at[zi, pl.ds(row0, C)], kc.at[0], sl.at[2]),
        pltpu.make_async_copy(v_hbm.at[:, zi, pl.ds(row0, C)], kc.at[pl.ds(1, 3)], sl.at[3]),
        pltpu.make_async_copy(c_hbm.at[:, k_from], kin.at[0, own, k_to], sl.at[4]),
        pltpu.make_async_copy(v_hbm.at[:, :, k_from], kin.at[pl.ds(1, 3), own, k_to], sl.at[5]),
    ]
    for copy in local:
        copy.start()

    @pl.when(group == 0)
    def _():
        ini[:, HALO : 2 * HALO] = jnp.zeros((zl, HALO, NX), jnp.float32)

    @pl.when(row0 + C == NY)
    def _():
        ini[:, WC : WC + HALO] = jnp.zeros((zl, HALO, NX), jnp.float32)

    @pl.when(band == 0)
    def _():
        kin[:, :, HALO : 2 * HALO] = jnp.zeros((4, NZ, HALO, NX), jnp.float32)

    @pl.when(band == bands - 1)
    def _():
        kin[:, :, RH : RH + HALO] = jnp.zeros((4, NZ, HALO, NX), jnp.float32)

    pl.semaphore_wait(barrier, T + S - 2)
    sent = []

    def send(source, target, ssem, rsem, tt, ts, valid=None, maybe_self=False):
        copy = remote(source, target, ssem, rsem, tt, ts)
        away = valid
        if maybe_self:
            same = jnp.logical_and(tt == t, ts == s)
            here = same if valid is None else jnp.logical_and(valid, same)
            away = jnp.logical_not(same)
            if valid is not None:
                away = jnp.logical_and(valid, away)

            @pl.when(here)
            def _():
                pltpu.make_async_copy(source, target, rsem).start()

        if away is None:
            copy.start()
            sent.append(copy.wait_send)
        else:

            @pl.when(away)
            def _():
                copy.start()

            def finish():
                @pl.when(away)
                def _():
                    copy.wait_send()

            sent.append(finish)

    def arrived(target, rsem, valid=None):
        if valid is None:
            pltpu.make_async_copy(target, target, rsem).wait()
        else:

            @pl.when(valid)
            def _():
                pltpu.make_async_copy(target, target, rsem).wait()

    local[0].wait()
    for m in range(T - 1, 0, -1):
        tt = t ^ m
        send(fbuf.at[chunk(tt)], times.at[t], s1.at[m], r1.at[m], tt, s)
    inner_rows = pl.ds(row0, C)
    up_s = jnp.minimum(s + 1, S - 1)
    down_s = jnp.maximum(s - 1, 0)
    send(i_hbm.at[zl - 1, inner_rows], edge.at[0], se.at[0], re.at[0], t, up_s, valid=s + 1 < S)
    send(i_hbm.at[0, inner_rows], edge.at[1], se.at[1], re.at[1], t, down_s, valid=s > 0)
    half = zl // 2
    share = (t % 2) * half
    rest = half - share
    partner = t ^ 1
    for m in range(1, S):
        ts = s ^ m
        from_rows, to_rows = space_window(ts)
        give = pl.ds(share, half)
        put = pl.ds(s * zl + share, half)
        send(c_hbm.at[give, from_rows], kin.at[0, put, to_rows], sk.at[m, 0], rk.at[m, 0], t, ts)
        send(v_hbm.at[:, give, from_rows], kin.at[pl.ds(1, 3), put, to_rows], sk.at[m, 1], rk.at[m, 1], t, ts)
    times[pl.ds(t, 1)] = fbuf[chunk(t)][None]
    for copy in local[1:]:
        copy.wait()

    def shifted(value, by, axis):
        return pltpu.roll(value, by % value.shape[axis], axis)

    column = lax.broadcasted_iota(jnp.int32, (C, NX), 1)
    arrived(edge.at[0], re.at[0], valid=s > 0)
    arrived(edge.at[1], re.at[1], valid=s + 1 < S)

    @pl.when(s == 0)
    def _():
        edge[0] = jnp.zeros((C, NX), jnp.float32)

    @pl.when(s + 1 == S)
    def _():
        edge[1] = jnp.zeros((C, NX), jnp.float32)

    inner = pl.ds(2 * HALO, C)
    wide = ini[zi, pl.ds(HALO, WC)]
    middle = wide[HALO : HALO + C]
    lower = jnp.where(zi == 0, edge[0], ini[jnp.maximum(zi - 1, 0), inner])
    upper = jnp.where(zi == zl - 1, edge[1], ini[jnp.minimum(zi + 1, zl - 1), inner])
    coupling = kc[0]
    adz = coupling * kc[1]
    ady = coupling * kc[2]
    adx = coupling * kc[3]
    summed = (coupling - adz) * upper + (coupling + adz) * lower
    summed += (coupling - ady) * shifted(wide, -1, 0)[HALO : HALO + C]
    summed += (coupling + ady) * shifted(wide, 1, 0)[HALO : HALO + C]
    summed += (coupling - adx) * jnp.where(column == NX - 1, 0.0, shifted(middle, -1, 1))
    summed += (coupling + adx) * jnp.where(column == 0, 0.0, shifted(middle, 1, 1))
    start = summed - 6.0 * coupling * middle

    for m in range(1, T):
        arrived(times.at[t ^ m], r1.at[m])

    for block in range(C // 8):
        rows = slice(block * 8, block * 8 + 8)
        spectrum = forward_transform([times[m, rows] + start[rows] for m in range(T)])
        for u in range(U):
            for p in range(2):
                fields[u, p, rows] = spectrum[u][p]

    kinds = ((0, R, HALO), (0, HALO, HALO + R), (R - HALO, HALO, 0))

    def lying(z, first, count):
        return land.at[:, pl.ds(pl.multiple_of(z * PS + first, 8), count)]

    for kind, m in [(0, m) for m in range(NZ - 1, -1, -1)] + [(k, m) for m in range(NZ - 1, -1, -1) for k in (1, 2)]:
        spot = at ^ m
        u = spot // q
        o = spot % q
        b = group * q + o
        if True:
            to = b + (0, -1, 1)[kind]
            valid = (None, to >= 0, to < bands)[kind]
            first, count, put = kinds[kind]
            source = fields.at[u, :, pl.ds(pl.multiple_of(o * R + first, 8), count)]
            if kind == 0 and m == 0:
                own_rows = pl.ds(pl.multiple_of(plane * PS + put, 8), count)
                land[:, own_rows] = fields[u, :, pl.ds(pl.multiple_of(o * R, 8), R)]
                continue
            to_t, to_s = place(u, jnp.clip(to, 0, bands - 1))
            send(
                source,
                lying(plane, put, count),
                s2.at[m, kind],
                r2.at[plane, kind],
                to_t,
                to_s,
                valid=valid,
                maybe_self=kind > 0 and q > 1,
            )

    for m in range(1, S):
        theirs = (s ^ m) * zl
        block_c = kin.at[0, pl.ds(theirs + share, half), k_to]
        block_v = kin.at[pl.ds(1, 3), pl.ds(theirs + share, half), k_to]
        arrived(block_c, rk.at[m, 0])
        arrived(block_v, rk.at[m, 1])
        send(block_c, block_c, sf.at[m, 0], rf.at[m, 0], partner, s)
        send(block_v, block_v, sf.at[m, 1], rf.at[m, 1], partner, s)
    for m in range(1, S):
        theirs = (s ^ m) * zl
        arrived(kin.at[0, pl.ds(theirs + rest, half), k_to], rf.at[m, 0])
        arrived(kin.at[pl.ds(1, 3), pl.ds(theirs + rest, half), k_to], rf.at[m, 1])

    angles = [2.0 * math.pi * u / U / 2 for u in range(U)]
    shift_re1 = by_index(unit, [rho * math.cos(a) for a in angles])
    shift_im1 = by_index(unit, [0.0] + [rho * math.sin(a) for a in angles[1:]])
    shift_re2 = by_index(unit, [-rho] + [rho * math.cos(a) for a in angles[1:]])
    z_at = lax.broadcasted_iota(jnp.int32, (NZ, NX), 0)
    x_at = lax.broadcasted_iota(jnp.int32, (NZ, NX), 1)

    def line(y):
        if isinstance(y, int):
            return pl.ds((y + O) * NZ, NZ)
        return pl.ds(pl.multiple_of((y + O) * NZ, 8), NZ)

    flat_kin = kin.reshape(4, NZ * PK, NX)

    @pl.loop(0, RH, unroll=4)
    def _(i):
        c, vz, vy, vx = [flat_kin[m, pl.ds(i + HALO, NZ, stride=PK)] for m in range(4)]
        to = line(i - HALO)
        az = c * vz
        ay = c * vy
        ax = c * vx
        zero = jnp.zeros_like(c)
        coef[0, to] = jnp.where(z_at == NZ - 1, zero, c - az)
        coef[1, to] = jnp.where(z_at == 0, zero, c + az)
        coef[2, to] = c - ay
        coef[3, to] = c + ay
        coef[4, to] = jnp.where(x_at == NX - 1, zero, c - ax)
        coef[5, to] = jnp.where(x_at == 0, zero, c + ax)
        diag1 = 1.0 + 6.0 * c - shift_re1
        diag2 = 1.0 + 6.0 * c - shift_re2
        im2 = shift_im1 * shift_im1
        modulus1 = diag1 * diag1 + im2
        modulus2 = diag2 * diag2 + im2
        pq[0, to] = diag1 / modulus1
        pq[1, to] = diag2 / modulus2
        pq[2, to] = shift_im1 / modulus1

    @pl.when(band == 0)
    def _():
        for z in range(NZ):
            land[:, z * PS : z * PS + HALO] = jnp.zeros((2, HALO, NX), jnp.float32)
        last[: HALO * NZ] = jnp.zeros((HALO * NZ, NX), jnp.float32)

    @pl.when(band == bands - 1)
    def _():
        for z in range(NZ):
            land[:, z * PS + HALO + R : z * PS + RH] = jnp.zeros((2, HALO, NX), jnp.float32)
        last[(HALO + R) * NZ :] = jnp.zeros((HALO * NZ, NX), jnp.float32)

    reach = -(-GUARD // R)
    counts = [min(R, GUARD - j * R) for j in range(reach)]
    for j in range(reach):
        spread = counts[j] * NZ

        @pl.when(band < j + 1)
        def _(j=j, spread=spread):
            first = (O - j * R - counts[j]) * NZ
            wc[:, first : first + spread] = jnp.zeros((2, spread, NX), jnp.float32)

        @pl.when(band + j + 1 > bands - 1)
        def _(j=j, spread=spread):
            first = (O + R + j * R) * NZ
            wc[:, first : first + spread] = jnp.zeros((2, spread, NX), jnp.float32)

    for m in range(NZ):
        z = plane ^ m
        if m:
            arrived(lying(z, HALO, R), r2.at[z, 0])
        arrived(lying(z, HALO + R, HALO), r2.at[z, 1], valid=band < bands - 1)
        arrived(lying(z, 0, HALO), r2.at[z, 2], valid=band > 0)

    def scaled(y, re_part, im_part):
        p1, p2, im = pq[0, line(y)], pq[1, line(y)], pq[2, line(y)]
        return re_part * p1 + im_part * im, im_part * p2 - re_part * im

    def neighbours(old, y, p):
        here = old[p, line(y)]
        total = src[p, line(y)] + coef[2, line(y)] * old[p, line(y + 1)] + coef[3, line(y)] * old[p, line(y - 1)]
        total += coef[0, line(y)] * shifted(here, -1, 0) + coef[1, line(y)] * shifted(here, 1, 0)
        total += coef[4, line(y)] * shifted(here, -1, 1) + coef[5, line(y)] * shifted(here, 1, 1)
        return total

    def sweep(old, new, low, high):
        for y in range(low, high):
            re_part, im_part = scaled(y, neighbours(old, y, 0), neighbours(old, y, 1))
            new[0, line(y)] = re_part
            new[1, line(y)] = im_part

    for y in range(-HALO, R + HALO):
        pair = [land[p, pl.ds(y + HALO, NZ, stride=PS)] for p in range(2)]
        src[0, line(y)] = pair[0]
        src[1, line(y)] = pair[1]
        re_part, im_part = scaled(y, *pair)
        wa[0, line(y)] = re_part
        wa[1, line(y)] = im_part
    old, new = wa, wb
    for k in range(1, SWEEPS):
        sweep(old, new, k - HALO, R + HALO - k)
        old, new = new, old
    weight = [2.0 * math.cos(2.0 * math.pi * u * (T - 1) / T) / T for u in range(U)]
    weight[0] = 1.0 / T
    other = [-2.0 * math.sin(2.0 * math.pi * u * (T - 1) / T) / T for u in range(U)]
    other[0] = (1.0 - 2.0 * ((T - 1) % 2)) / T
    weight_re = by_index(unit, [rho * w for w in weight])
    weight_im = by_index(unit, [rho * w for w in other])
    for y in range(R):
        re_part, im_part = scaled(y, neighbours(old, y, 0), neighbours(old, y, 1))
        wc[0, line(y)] = re_part
        wc[1, line(y)] = im_part
        part[y * NZ : y * NZ + NZ] = weight_re * re_part + weight_im * im_part

    def piece(u):
        return pl.ds(pl.multiple_of(u * chunk_rows, 8), chunk_rows)

    for m in range(U - 1, 0, -1):
        u = unit ^ m
        send(part.at[piece(u)], gathered.at[m], ss.at[m], rs.at[m], *place(u, band))

    def span(first, count):
        return pl.ds((first + O) * NZ, count * NZ)

    for j in range(reach):
        count = counts[j]
        above = jnp.minimum(band + j + 1, bands - 1)
        below = jnp.maximum(band - j - 1, 0)
        to_above = wc.at[:, span(-j * R - count, count)]
        to_below = wc.at[:, span(R + j * R, count)]
        source = wc.at[:, span(R - count, count)]
        send(source, to_above, sw.at[j, 0], rw.at[j, 0], *place(unit, above), valid=band + j + 1 < bands)
        source = wc.at[:, span(0, count)]
        send(source, to_below, sw.at[j, 1], rw.at[j, 1], *place(unit, below), valid=band >= j + 1)
    earlier = list(sent)
    sent.clear()
    for m in range(1, U):
        arrived(gathered.at[m], rs.at[m])
    total = part[piece(unit)]
    for m in range(1, U):
        total = total + gathered[m]
    reduced[...] = total
    base = HALO * NZ
    mine = pl.ds(pl.multiple_of(base + unit * chunk_rows, 8), chunk_rows)
    last[mine] = total
    low_at = pl.ds(pl.multiple_of((HALO + R) * NZ + jnp.minimum(unit, edges - 1) * chunk_rows, 8), chunk_rows)
    high_at = pl.ds(pl.multiple_of(jnp.maximum(unit - (U - edges), 0) * chunk_rows, 8), chunk_rows)
    goes_down = jnp.logical_and(band > 0, unit < edges)
    goes_up = jnp.logical_and(band < bands - 1, unit >= U - edges)
    for m in range(U - 1, -1, -1):
        u = unit ^ m
        below = place(u, jnp.maximum(band - 1, 0))
        above = place(u, jnp.minimum(band + 1, bands - 1))
        send(reduced, last.at[low_at], sg.at[m, 1], rg.at[m, 1], *below, valid=goes_down)
        send(reduced, last.at[high_at], sg.at[m, 2], rg.at[m, 2], *above, valid=goes_up)
        if m:
            send(reduced, last.at[mine], sg.at[m, 0], rg.at[m, 0], *place(u, band))
    for j in range(reach):
        count = counts[j]
        arrived(wc.at[:, span(-j * R - count, count)], rw.at[j, 0], valid=band >= j + 1)
        arrived(wc.at[:, span(R + j * R, count)], rw.at[j, 1], valid=band + j + 1 < bands)
    for y in range(-HALO, R + HALO):
        wa[0, line(y)] = neighbours(wc, y, 0)
        wa[1, line(y)] = neighbours(wc, y, 1)
    for finish in earlier:
        finish()
    for m in range(U):
        u = unit ^ m
        if m:
            arrived(last.at[pl.ds(pl.multiple_of(base + u * chunk_rows, 8), chunk_rows)], rg.at[m, 0])
        here = pl.ds(pl.multiple_of((HALO + R) * NZ + jnp.minimum(u, edges - 1) * chunk_rows, 8), chunk_rows)
        arrived(last.at[here], rg.at[m, 1], valid=jnp.logical_and(band < bands - 1, u < edges))
        here = pl.ds(pl.multiple_of(jnp.maximum(u - (U - edges), 0) * chunk_rows, 8), chunk_rows)
        arrived(last.at[here], rg.at[m, 2], valid=jnp.logical_and(band > 0, u >= U - edges))

    both = jnp.where(unit == 0, jnp.float32(1.0), jnp.float32(0.0))
    for y in range(-HALO, R + HALO):
        wrap = last[(y + HALO) * NZ : (y + HALO + 1) * NZ]
        wrap_im = wrap * both
        src[0, line(y)] = src[0, line(y)] - wrap
        src[1, line(y)] = src[1, line(y)] - wrap_im
        re_part, im_part = scaled(y, wa[0, line(y)] - wrap, wa[1, line(y)] - wrap_im)
        wb[0, line(y)] = re_part
        wb[1, line(y)] = im_part
    old, new = wb, wa
    for k in range(2, SWEEPS + 1):
        sweep(old, new, k - GUARD, R + GUARD - k)
        old, new = new, old
    for y in range(R):
        re_part, im_part = scaled(y, neighbours(old, y, 0), neighbours(old, y, 1))
        fin[0, pl.ds(y, NZ, stride=PF)] = re_part
        fin[1, pl.ds(y, NZ, stride=PF)] = im_part

    offset = pl.multiple_of((band % q) * R, 8)
    for m in range(NZ - 1, -1, -1):
        z = plane ^ m
        source = pl.ds(pl.multiple_of(z * PF, 8), R)
        if m == 0:
            back[pl.ds(unit, 1), :, pl.ds(offset, R)] = fin[:, source][None]
            continue
        send(
            fin.at[:, source],
            back.at[unit, :, pl.ds(offset, R)],
            s3.at[m],
            r3.at[unit, band % q],
            group * zl + z % zl,
            z // zl,
        )
    for m in range(1, U * q):
        spot = at ^ m
        u = spot // q
        o = spot % q
        arrived(back.at[u, :, pl.ds(pl.multiple_of(o * R, 8), R)], r3.at[u, o])
    for block in range(C // 8):
        rows = slice(block * 8, block * 8 + 8)
        result = inverse_transform([(back[u, 0, rows], back[u, 1, rows]) for u in range(U)], middle[rows])
        for m in range(T):
            states[m, rows] = result[m]
    for m in range(1, T):
        tt = lax.rem(t + m, T)
        send(states.at[tt], out_ref.at[chunk(t)], s4.at[m], r4.at[m], tt, s)
    out_ref[chunk(t)] = states[pl.ds(t, 1)][0]
    for finish in sent:
        finish()
    for m in range(1, T):
        arrived(out_ref.at[chunk(lax.rem(t + T - m, T))], r4.at[m])


def body(forcing, initial, coupling, velocity):
    local_steps, zl, NY, NX = forcing.shape
    T = lax.axis_size("tm")
    S = lax.axis_size("space")
    U = T // 2
    NZ = zl * S
    C = zl * NY // T
    bands = 2 * S
    R = NY // bands
    RH = R + 2 * HALO
    WC = C + 2 * HALO
    q = C // R
    PK = RH + 3 * HALO
    PS = RH + HALO
    PF = R + HALO
    rows = R + 2 * GUARD
    reach = -(-GUARD // R)
    assert local_steps == 1 and SWEEPS == HALO <= R and ITERS == 2
    assert S % q == 0 and zl % 2 == 0 and T % 4 == 0
    assert C % R == 0 and NY % C == 0 and U * q == NZ and NZ % 8 == 0
    assert T & (T - 1) == 0 and S & (S - 1) == 0 and NZ & (NZ - 1) == 0
    assert (R * NZ // U) % 8 == 0 and (HALO * U) % R == 0 and WC <= NY
    f32 = jnp.float32
    dma = pltpu.SemaphoreType.DMA
    hbm = pl.BlockSpec(memory_space=pltpu.HBM)
    out = pl.pallas_call(
        lambda *refs: kernel((T, S, NY, NX, zl), *refs),
        out_shape=jax.ShapeDtypeStruct((zl * NY, NX), f32),
        in_specs=[hbm] * 4,
        out_specs=pl.BlockSpec(memory_space=pltpu.VMEM),
        scratch_shapes=[
            pltpu.VMEM((zl * NY, NX), f32),
            pltpu.VMEM((zl, WC + 2 * HALO, NX), f32),
            pltpu.VMEM((4, C, NX), f32),
            pltpu.VMEM((T, C, NX), f32),
            pltpu.VMEM((U, 2, C, NX), f32),
            pltpu.VMEM((2, C, NX), f32),
            pltpu.VMEM((4, NZ, PK, NX), f32),
            pltpu.VMEM((6, rows * NZ, NX), f32),
            pltpu.VMEM((3, rows * NZ, NX), f32),
            pltpu.VMEM((2, NZ * PS, NX), f32),
            pltpu.VMEM((2, rows * NZ, NX), f32),
            pltpu.VMEM((2, rows * NZ, NX), f32),
            pltpu.VMEM((2, rows * NZ, NX), f32),
            pltpu.VMEM((2, rows * NZ, NX), f32),
            pltpu.VMEM((R * NZ, NX), f32),
            pltpu.VMEM((U, R * NZ // U, NX), f32),
            pltpu.VMEM((R * NZ // U, NX), f32),
            pltpu.VMEM((RH * NZ, NX), f32),
            pltpu.VMEM((2, NZ * PF, NX), f32),
            pltpu.VMEM((U, 2, C, NX), f32),
            pltpu.VMEM((T, C, NX), f32),
            dma((6,)),
            dma((T,)),
            dma((T,)),
            dma((NZ, 3)),
            dma((NZ, 3)),
            dma((S, 2)),
            dma((S, 2)),
            dma((S, 2)),
            dma((S, 2)),
            dma((2,)),
            dma((2,)),
            dma((reach, 2)),
            dma((reach, 2)),
            dma((U,)),
            dma((U,)),
            dma((U, 3)),
            dma((U, 3)),
            dma((NZ,)),
            dma((U, q)),
            dma((T,)),
            dma((T,)),
        ],
        compiler_params=pltpu.CompilerParams(
            has_side_effects=True, collective_id=0, vmem_limit_bytes=48 * 1024 * 1024
        ),
    )(*[pltpu.with_memory_space_constraint(a, pltpu.HBM) for a in (forcing.reshape(zl * NY, NX), initial, coupling, velocity)])
    return out.reshape(forcing.shape)


def solution(mesh):
    return jax.shard_map(
        body,
        mesh=mesh,
        in_specs=(
            P("tm", "space", None, None),
            P("space", None, None),
            P("space", None, None),
            P(None, "space", None, None),
        ),
        out_specs=P("tm", "space", None, None),
        check_vma=False,
    )
```

```python
import math

import jax
import jax.numpy as jnp
import numpy as np
from jax import lax
from jax.experimental import pallas as pl
from jax.experimental.pallas import tpu as pltpu
from jax.sharding import PartitionSpec as P

ITERS = 2
SWEEPS = 8
HALO = 8
GUARD = SWEEPS + 1

wrap_alpha = 0.1


def by_index(index, values):
    picked = jnp.float32(values[0])
    for at in range(1, len(values)):
        picked = jnp.where(index == at, jnp.float32(values[at]), picked)
    return picked


def weighted(terms):
    total = None
    for weight, value in terms:
        if abs(weight) < 1e-12:
            continue
        if abs(weight - 1.0) < 1e-12:
            term = value
        elif abs(weight + 1.0) < 1e-12:
            term = None
            total = -value if total is None else total - value
        else:
            term = value * float(weight)
        if term is not None:
            total = term if total is None else total + term
    return total


def plus(first, second):
    return second if first is None else first if second is None else first + second


def minus(first, second):
    return first if second is None else -second if first is None else first - second


def forward_transform(values):
    T = len(values)
    U = T // 2
    gamma = [wrap_alpha ** (n / T) for n in range(T)]
    a = [values[n] if n == 0 else values[n] * float(gamma[n]) for n in range(T)]
    even = {n: a[n] + a[T - n] for n in range(1, U)}
    odd = {n: a[n] - a[T - n] for n in range(1, U)}

    def cosine(u, parity):
        return weighted([(math.cos(2 * math.pi * u * n / T), even[n]) for n in range(1, U) if n % 2 == parity])

    def sine(u, parity):
        return weighted([(math.sin(2 * math.pi * u * n / T), odd[n]) for n in range(1, U) if n % 2 == parity])

    result = [None] * U
    ends = [a[0] + a[U], a[0] - a[U]]
    zero_even = plus(ends[0], cosine(0, 0))
    zero_odd = cosine(0, 1)
    result[0] = (plus(zero_even, zero_odd), minus(zero_even, zero_odd))
    for u in range(1, U // 2 + 1):
        c_even = plus(ends[u % 2], cosine(u, 0))
        c_odd = cosine(u, 1)
        s_even, s_odd = sine(u, 0), sine(u, 1)
        if u == U - u:
            result[u] = (plus(c_even, c_odd), minus(None, plus(s_even, s_odd)))
            continue
        result[u] = (plus(c_even, c_odd), minus(None, plus(s_even, s_odd)))
        result[U - u] = (minus(c_even, c_odd), minus(s_even, s_odd))
    return result


def inverse_transform(pairs, begin):
    U = len(pairs)
    T = 2 * U
    scale = [1.0 / (T * wrap_alpha ** (m / T)) for m in range(T)]
    first, middle = pairs[0]
    ends = [first + middle, first - middle]

    def cosine(m, parity):
        return weighted([(2 * math.cos(2 * math.pi * u * m / T), pairs[u][0]) for u in range(1, U) if u % 2 == parity])

    def sine(m, parity):
        return weighted([(2 * math.sin(2 * math.pi * u * m / T), pairs[u][1]) for u in range(1, U) if u % 2 == parity])

    result = [None] * T

    def put(m, real, imaginary):
        for at, value in ((m, minus(real, imaginary)), ((T - m) % T, plus(real, imaginary))):
            if result[at] is None:
                result[at] = begin + value * float(scale[at])

    for m in range(0, U // 2 + 1):
        c_even, c_odd = plus(ends[m % 2], cosine(m, 0)), cosine(m, 1)
        s_even, s_odd = sine(m, 0), sine(m, 1)
        put(m, plus(c_even, c_odd), plus(s_even, s_odd))
        other = U - m
        if other != m:
            put(other, minus(c_even, c_odd), minus(s_odd, s_even))
    return result


def kernel(
    dims,
    f_hbm,
    i_hbm,
    c_hbm,
    v_hbm,
    out_ref,
    fbuf,
    ini,
    kc,
    times,
    fields,
    edge,
    kin,
    coef,
    pq,
    land,
    src,
    wa,
    wb,
    wc,
    part,
    gathered,
    reduced,
    last,
    fin,
    back,
    states,
    sl,
    s1,
    r1,
    s2,
    r2,
    sk,
    rk,
    sf,
    rf,
    se,
    re,
    sw,
    rw,
    ss,
    rs,
    sg,
    rg,
    s3,
    r3,
    s4,
    r4,
):
    T, S, NY, NX, zl = dims
    U = T // 2
    NZ = zl * S
    C = zl * NY // T
    bands = 2 * S
    R = NY // bands
    RH = R + 2 * HALO
    WC = C + 2 * HALO
    q = C // R
    PK = RH + 3 * HALO
    PS = RH + HALO
    PF = R + HALO
    chunk_rows = R * NZ // U
    edges = HALO * U // R
    rho = wrap_alpha ** (1.0 / T)
    O = GUARD

    t = lax.axis_index("tm")
    s = lax.axis_index("space")
    group = t // zl
    zi = t % zl
    at = zi * S + s
    unit = at // q
    band = group * q + at % q
    plane = s * zl + zi
    row0 = pl.multiple_of(group * C, 8)

    def place(u, b):
        spot = u * q + b % q
        return (b // q) * zl + spot // S, spot % S

    def chunk(tt):
        start = (tt % zl) * NY + (tt // zl) * C
        return pl.ds(pl.multiple_of(start, 8), C)

    def device(tt, ts):
        return {"tm": tt, "space": ts}

    def remote(source, target, ssem, rsem, tt, ts):
        return pltpu.make_async_remote_copy(
            src_ref=source,
            dst_ref=target,
            send_sem=ssem,
            recv_sem=rsem,
            device_id=device(tt, ts),
            device_id_type=pl.DeviceIdType.MESH,
        )

    barrier = pltpu.get_barrier_semaphore()
    for m in range(T - 1, 0, -1):
        pl.semaphore_signal(barrier, inc=1, device_id=device(t ^ m, s), device_id_type=pl.DeviceIdType.MESH)
    for m in range(1, S):
        pl.semaphore_signal(barrier, inc=1, device_id=device(t, s ^ m), device_id_type=pl.DeviceIdType.MESH)

    def window(start, count):
        first = jnp.clip(start - HALO, 0, NY - count)
        offset = HALO + first - (start - HALO)
        return pl.ds(pl.multiple_of(first, 8), count), pl.ds(pl.multiple_of(offset, 8), count)

    def space_window(ts):
        return window((group * q + (zi * S + ts) % q) * R, RH)

    own = pl.ds(s * zl, zl)
    k_from, k_to = space_window(s)
    i_from, i_to = window(row0, WC)
    local = [
        pltpu.make_async_copy(f_hbm, fbuf, sl.at[0]),
        pltpu.make_async_copy(i_hbm.at[:, i_from], ini.at[:, i_to], sl.at[1]),
        pltpu.make_async_copy(c_hbm.at[zi, pl.ds(row0, C)], kc.at[0], sl.at[2]),
        pltpu.make_async_copy(v_hbm.at[:, zi, pl.ds(row0, C)], kc.at[pl.ds(1, 3)], sl.at[3]),
        pltpu.make_async_copy(c_hbm.at[:, k_from], kin.at[0, own, k_to], sl.at[4]),
        pltpu.make_async_copy(v_hbm.at[:, :, k_from], kin.at[pl.ds(1, 3), own, k_to], sl.at[5]),
    ]
    for copy in local:
        copy.start()

    @pl.when(group == 0)
    def _():
        ini[:, HALO : 2 * HALO] = jnp.zeros((zl, HALO, NX), jnp.float32)

    @pl.when(row0 + C == NY)
    def _():
        ini[:, WC : WC + HALO] = jnp.zeros((zl, HALO, NX), jnp.float32)

    @pl.when(band == 0)
    def _():
        kin[:, :, HALO : 2 * HALO] = jnp.zeros((4, NZ, HALO, NX), jnp.float32)

    @pl.when(band == bands - 1)
    def _():
        kin[:, :, RH : RH + HALO] = jnp.zeros((4, NZ, HALO, NX), jnp.float32)

    pl.semaphore_wait(barrier, T + S - 2)
    sent = []

    def send(source, target, ssem, rsem, tt, ts, valid=None, maybe_self=False):
        copy = remote(source, target, ssem, rsem, tt, ts)
        away = valid
        if maybe_self:
            same = jnp.logical_and(tt == t, ts == s)
            here = same if valid is None else jnp.logical_and(valid, same)
            away = jnp.logical_not(same)
            if valid is not None:
                away = jnp.logical_and(valid, away)

            @pl.when(here)
            def _():
                pltpu.make_async_copy(source, target, rsem).start()

        if away is None:
            copy.start()
            sent.append(copy.wait_send)
        else:

            @pl.when(away)
            def _():
                copy.start()

            def finish():
                @pl.when(away)
                def _():
                    copy.wait_send()

            sent.append(finish)

    def send_all(copies, valid):
        copies = [remote(*copy) for copy in copies]

        @pl.when(valid)
        def _():
            for copy in copies:
                copy.start()

        def finish():
            @pl.when(valid)
            def _():
                for copy in copies:
                    copy.wait_send()

        sent.append(finish)

    def arrived_all(pairs, valid):
        @pl.when(valid)
        def _():
            for target, rsem in pairs:
                pltpu.make_async_copy(target, target, rsem).wait()

    def arrived(target, rsem, valid=None):
        if valid is None:
            pltpu.make_async_copy(target, target, rsem).wait()
        else:

            @pl.when(valid)
            def _():
                pltpu.make_async_copy(target, target, rsem).wait()

    local[0].wait()
    for m in range(T - 1, 0, -1):
        tt = t ^ m
        send(fbuf.at[chunk(tt)], times.at[t], s1.at[m], r1.at[m], tt, s)
    inner_rows = pl.ds(row0, C)
    up_s = jnp.minimum(s + 1, S - 1)
    down_s = jnp.maximum(s - 1, 0)
    send(i_hbm.at[zl - 1, inner_rows], edge.at[0], se.at[0], re.at[0], t, up_s, valid=s + 1 < S)
    send(i_hbm.at[0, inner_rows], edge.at[1], se.at[1], re.at[1], t, down_s, valid=s > 0)
    half = zl // 2
    share = (t % 2) * half
    rest = half - share
    partner = t ^ 1
    for m in range(1, S):
        ts = s ^ m
        from_rows, to_rows = space_window(ts)
        give = pl.ds(share, half)
        put = pl.ds(s * zl + share, half)
        send(c_hbm.at[give, from_rows], kin.at[0, put, to_rows], sk.at[m, 0], rk.at[m, 0], t, ts)
        send(v_hbm.at[:, give, from_rows], kin.at[pl.ds(1, 3), put, to_rows], sk.at[m, 1], rk.at[m, 1], t, ts)
    times[pl.ds(t, 1)] = fbuf[chunk(t)][None]
    for copy in local[1:]:
        copy.wait()

    def shifted(value, by, axis):
        return pltpu.roll(value, by % value.shape[axis], axis)

    column = lax.broadcasted_iota(jnp.int32, (C, NX), 1)
    arrived(edge.at[0], re.at[0], valid=s > 0)
    arrived(edge.at[1], re.at[1], valid=s + 1 < S)

    @pl.when(s == 0)
    def _():
        edge[0] = jnp.zeros((C, NX), jnp.float32)

    @pl.when(s + 1 == S)
    def _():
        edge[1] = jnp.zeros((C, NX), jnp.float32)

    inner = pl.ds(2 * HALO, C)
    wide = ini[zi, pl.ds(HALO, WC)]
    middle = wide[HALO : HALO + C]
    lower = jnp.where(zi == 0, edge[0], ini[jnp.maximum(zi - 1, 0), inner])
    upper = jnp.where(zi == zl - 1, edge[1], ini[jnp.minimum(zi + 1, zl - 1), inner])
    coupling = kc[0]
    adz = coupling * kc[1]
    ady = coupling * kc[2]
    adx = coupling * kc[3]
    summed = (coupling - adz) * upper + (coupling + adz) * lower
    summed += (coupling - ady) * shifted(wide, -1, 0)[HALO : HALO + C]
    summed += (coupling + ady) * shifted(wide, 1, 0)[HALO : HALO + C]
    summed += (coupling - adx) * jnp.where(column == NX - 1, 0.0, shifted(middle, -1, 1))
    summed += (coupling + adx) * jnp.where(column == 0, 0.0, shifted(middle, 1, 1))
    start = summed - 6.0 * coupling * middle

    for m in range(1, T):
        arrived(times.at[t ^ m], r1.at[m])

    for block in range(C // 8):
        rows = slice(block * 8, block * 8 + 8)
        spectrum = forward_transform([times[m, rows] + start[rows] for m in range(T)])
        for u in range(U):
            for p in range(2):
                fields[u, p, rows] = spectrum[u][p]

    kinds = ((0, R, HALO), (0, HALO, HALO + R), (R - HALO, HALO, 0))

    def lying(z, first, count):
        return land.at[:, pl.ds(pl.multiple_of(z * PS + first, 8), count)]

    def spectra(m, kind):
        spot = at ^ m
        u = spot // q
        o = spot % q
        to = group * q + o + (0, -1, 1)[kind]
        valid = (None, to >= 0, to < bands)[kind]
        first, count, put = kinds[kind]
        source = fields.at[u, :, pl.ds(pl.multiple_of(o * R + first, 8), count)]
        target = lying(plane, put, count)
        to_t, to_s = place(u, jnp.clip(to, 0, bands - 1))
        return (source, target, s2.at[m, kind], r2.at[plane, kind], to_t, to_s), valid

    for m in range(NZ - 1, 0, -1):
        copy, _ = spectra(m, 0)
        send(*copy)
    own_rows = pl.ds(pl.multiple_of(plane * PS + HALO, 8), R)
    land[:, own_rows] = fields[unit, :, pl.ds(pl.multiple_of((band % q) * R, 8), R)]
    for kind in (1, 2):
        copies = [spectra(m, kind) for m in range(NZ - 1, -1, -1)]
        if q == 1:
            send_all([copy for copy, _ in copies], copies[0][1])
        else:
            for copy, valid in copies:
                send(*copy, valid=valid, maybe_self=True)

    for m in range(1, S):
        theirs = (s ^ m) * zl
        block_c = kin.at[0, pl.ds(theirs + share, half), k_to]
        block_v = kin.at[pl.ds(1, 3), pl.ds(theirs + share, half), k_to]
        arrived(block_c, rk.at[m, 0])
        arrived(block_v, rk.at[m, 1])
        send(block_c, block_c, sf.at[m, 0], rf.at[m, 0], partner, s)
        send(block_v, block_v, sf.at[m, 1], rf.at[m, 1], partner, s)
    for m in range(1, S):
        theirs = (s ^ m) * zl
        arrived(kin.at[0, pl.ds(theirs + rest, half), k_to], rf.at[m, 0])
        arrived(kin.at[pl.ds(1, 3), pl.ds(theirs + rest, half), k_to], rf.at[m, 1])

    angles = [2.0 * math.pi * u / U / 2 for u in range(U)]
    shift_re1 = by_index(unit, [rho * math.cos(a) for a in angles])
    shift_im1 = by_index(unit, [0.0] + [rho * math.sin(a) for a in angles[1:]])
    shift_re2 = by_index(unit, [-rho] + [rho * math.cos(a) for a in angles[1:]])
    z_at = lax.broadcasted_iota(jnp.int32, (NZ, NX), 0)
    x_at = lax.broadcasted_iota(jnp.int32, (NZ, NX), 1)

    def line(y):
        if isinstance(y, int):
            return pl.ds((y + O) * NZ, NZ)
        return pl.ds(pl.multiple_of((y + O) * NZ, 8), NZ)

    flat_kin = kin.reshape(4, NZ * PK, NX)

    @pl.loop(0, RH, unroll=4)
    def _(i):
        c, vz, vy, vx = [flat_kin[m, pl.ds(i + HALO, NZ, stride=PK)] for m in range(4)]
        to = line(i - HALO)
        az = c * vz
        ay = c * vy
        ax = c * vx
        zero = jnp.zeros_like(c)
        coef[0, to] = jnp.where(z_at == NZ - 1, zero, c - az)
        coef[1, to] = jnp.where(z_at == 0, zero, c + az)
        coef[2, to] = c - ay
        coef[3, to] = c + ay
        coef[4, to] = jnp.where(x_at == NX - 1, zero, c - ax)
        coef[5, to] = jnp.where(x_at == 0, zero, c + ax)
        diag1 = 1.0 + 6.0 * c - shift_re1
        diag2 = 1.0 + 6.0 * c - shift_re2
        im2 = shift_im1 * shift_im1
        modulus1 = diag1 * diag1 + im2
        modulus2 = diag2 * diag2 + im2
        pq[0, to] = diag1 / modulus1
        pq[1, to] = diag2 / modulus2
        pq[2, to] = shift_im1 / modulus1

    @pl.when(band == 0)
    def _():
        for z in range(NZ):
            land[:, z * PS : z * PS + HALO] = jnp.zeros((2, HALO, NX), jnp.float32)
        last[: HALO * NZ] = jnp.zeros((HALO * NZ, NX), jnp.float32)

    @pl.when(band == bands - 1)
    def _():
        for z in range(NZ):
            land[:, z * PS + HALO + R : z * PS + RH] = jnp.zeros((2, HALO, NX), jnp.float32)
        last[(HALO + R) * NZ :] = jnp.zeros((HALO * NZ, NX), jnp.float32)

    reach = -(-GUARD // R)
    counts = [min(R, GUARD - j * R) for j in range(reach)]
    for j in range(reach):
        spread = counts[j] * NZ

        @pl.when(band < j + 1)
        def _(j=j, spread=spread):
            first = (O - j * R - counts[j]) * NZ
            wc[:, first : first + spread] = jnp.zeros((2, spread, NX), jnp.float32)

        @pl.when(band + j + 1 > bands - 1)
        def _(j=j, spread=spread):
            first = (O + R + j * R) * NZ
            wc[:, first : first + spread] = jnp.zeros((2, spread, NX), jnp.float32)

    for m in range(1, NZ):
        z = plane ^ m
        arrived(lying(z, HALO, R), r2.at[z, 0])

    def scaled(y, re_part, im_part):
        p1, p2, im = pq[0, line(y)], pq[1, line(y)], pq[2, line(y)]
        return re_part * p1 + im_part * im, im_part * p2 - re_part * im

    def neighbours(old, y, p):
        here = old[p, line(y)]
        total = src[p, line(y)] + coef[2, line(y)] * old[p, line(y + 1)] + coef[3, line(y)] * old[p, line(y - 1)]
        total += coef[0, line(y)] * shifted(here, -1, 0) + coef[1, line(y)] * shifted(here, 1, 0)
        total += coef[4, line(y)] * shifted(here, -1, 1) + coef[5, line(y)] * shifted(here, 1, 1)
        return total

    def whole(j):
        return list(range(j - HALO, R + HALO - j))

    def within(j):
        return list(range(j, R - j))

    def around(j):
        return [y for y in range(j - HALO, R + HALO - j) if y not in range(j, R - j)]

    def update(old, new, y):
        re_part, im_part = scaled(y, neighbours(old, y, 0), neighbours(old, y, 1))
        new[0, line(y)] = re_part
        new[1, line(y)] = im_part

    weight = [2.0 * math.cos(2.0 * math.pi * u * (T - 1) / T) / T for u in range(U)]
    weight[0] = 1.0 / T
    other = [-2.0 * math.sin(2.0 * math.pi * u * (T - 1) / T) / T for u in range(U)]
    other[0] = (1.0 - 2.0 * ((T - 1) % 2)) / T
    weight_re = by_index(unit, [rho * w for w in weight])
    weight_im = by_index(unit, [rho * w for w in other])

    def solve_first(rows):
        for y in rows(0):
            pair = [land[p, pl.ds(y + HALO, NZ, stride=PS)] for p in range(2)]
            src[0, line(y)] = pair[0]
            src[1, line(y)] = pair[1]
            re_part, im_part = scaled(y, *pair)
            wa[0, line(y)] = re_part
            wa[1, line(y)] = im_part
        old, new = wa, wb
        for j in range(1, SWEEPS):
            for y in rows(j):
                update(old, new, y)
            old, new = new, old
        for y in rows(SWEEPS):
            re_part, im_part = scaled(y, neighbours(old, y, 0), neighbours(old, y, 1))
            wc[0, line(y)] = re_part
            wc[1, line(y)] = im_part
            part[y * NZ : y * NZ + NZ] = weight_re * re_part + weight_im * im_part

    uppers = [(lying(z, HALO + R, HALO), r2.at[z, 1]) for z in range(NZ)]
    lowers = [(lying(z, 0, HALO), r2.at[z, 2]) for z in range(NZ)]
    arrived_all(uppers, band < bands - 1)
    arrived_all(lowers, band > 0)
    solve_first(whole)

    def piece(u):
        return pl.ds(pl.multiple_of(u * chunk_rows, 8), chunk_rows)

    for m in range(U - 1, 0, -1):
        u = unit ^ m
        send(part.at[piece(u)], gathered.at[m], ss.at[m], rs.at[m], *place(u, band))

    def span(first, count):
        return pl.ds((first + O) * NZ, count * NZ)

    for j in range(reach):
        count = counts[j]
        above = jnp.minimum(band + j + 1, bands - 1)
        below = jnp.maximum(band - j - 1, 0)
        to_above = wc.at[:, span(-j * R - count, count)]
        to_below = wc.at[:, span(R + j * R, count)]
        source = wc.at[:, span(R - count, count)]
        send(source, to_above, sw.at[j, 0], rw.at[j, 0], *place(unit, above), valid=band + j + 1 < bands)
        source = wc.at[:, span(0, count)]
        send(source, to_below, sw.at[j, 1], rw.at[j, 1], *place(unit, below), valid=band >= j + 1)
    earlier = list(sent)
    sent.clear()
    for m in range(1, U):
        arrived(gathered.at[m], rs.at[m])
    total = part[piece(unit)]
    for m in range(1, U):
        total = total + gathered[m]
    reduced[...] = total
    base = HALO * NZ
    mine = pl.ds(pl.multiple_of(base + unit * chunk_rows, 8), chunk_rows)
    last[mine] = total
    low_at = pl.ds(pl.multiple_of((HALO + R) * NZ + jnp.minimum(unit, edges - 1) * chunk_rows, 8), chunk_rows)
    high_at = pl.ds(pl.multiple_of(jnp.maximum(unit - (U - edges), 0) * chunk_rows, 8), chunk_rows)
    goes_down = jnp.logical_and(band > 0, unit < edges)
    goes_up = jnp.logical_and(band < bands - 1, unit >= U - edges)
    low_sem = rg.at[jnp.minimum(unit, edges - 1), 1]
    high_sem = rg.at[jnp.maximum(unit - (U - edges), 0), 2]
    for m in range(U - 1, 0, -1):
        send(reduced, last.at[mine], sg.at[m, 0], rg.at[m, 0], *place(unit ^ m, band))
    order = range(U - 1, -1, -1)
    below = jnp.maximum(band - 1, 0)
    above = jnp.minimum(band + 1, bands - 1)
    send_all([(reduced, last.at[low_at], sg.at[m, 1], low_sem, *place(unit ^ m, below)) for m in order], goes_down)
    send_all([(reduced, last.at[high_at], sg.at[m, 2], high_sem, *place(unit ^ m, above)) for m in order], goes_up)
    for j in range(reach):
        count = counts[j]
        arrived(wc.at[:, span(-j * R - count, count)], rw.at[j, 0], valid=band >= j + 1)
        arrived(wc.at[:, span(R + j * R, count)], rw.at[j, 1], valid=band + j + 1 < bands)
    for y in range(-HALO, R + HALO):
        wa[0, line(y)] = neighbours(wc, y, 0)
        wa[1, line(y)] = neighbours(wc, y, 1)
    for finish in earlier:
        finish()
    for m in range(1, U):
        u = unit ^ m
        arrived(last.at[pl.ds(pl.multiple_of(base + u * chunk_rows, 8), chunk_rows)], rg.at[m, 0])

    both = jnp.where(unit == 0, jnp.float32(1.0), jnp.float32(0.0))

    def solve_second(rows):
        for y in rows(0):
            wrap = last[(y + HALO) * NZ : (y + HALO + 1) * NZ]
            wrap_im = wrap * both
            src[0, line(y)] = src[0, line(y)] - wrap
            src[1, line(y)] = src[1, line(y)] - wrap_im
            re_part, im_part = scaled(y, wa[0, line(y)] - wrap, wa[1, line(y)] - wrap_im)
            wb[0, line(y)] = re_part
            wb[1, line(y)] = im_part
        old, new = wb, wa
        for j in range(1, SWEEPS):
            for y in rows(j):
                update(old, new, y)
            old, new = new, old
        for y in rows(SWEEPS):
            re_part, im_part = scaled(y, neighbours(old, y, 0), neighbours(old, y, 1))
            fin[0, pl.ds(y, NZ, stride=PF)] = re_part
            fin[1, pl.ds(y, NZ, stride=PF)] = im_part

    tops = [(last.at[pl.ds((HALO + R) * NZ + e * chunk_rows, chunk_rows)], rg.at[e, 1]) for e in range(edges)]
    bottoms = [(last.at[pl.ds(e * chunk_rows, chunk_rows)], rg.at[e, 2]) for e in range(edges)]
    arrived_all(tops, band < bands - 1)
    arrived_all(bottoms, band > 0)
    solve_second(whole)

    offset = pl.multiple_of((band % q) * R, 8)
    earlier = list(sent)
    sent.clear()
    for m in range(NZ - 1, -1, -1):
        z = plane ^ m
        source = pl.ds(pl.multiple_of(z * PF, 8), R)
        if m == 0:
            back[pl.ds(unit, 1), :, pl.ds(offset, R)] = fin[:, source][None]
            continue
        send(
            fin.at[:, source],
            back.at[unit, :, pl.ds(offset, R)],
            s3.at[m],
            r3.at[unit, band % q],
            group * zl + z % zl,
            z // zl,
        )
    for finish in earlier:
        finish()
    for m in range(1, U * q):
        spot = at ^ m
        u = spot // q
        o = spot % q
        arrived(back.at[u, :, pl.ds(pl.multiple_of(o * R, 8), R)], r3.at[u, o])
    for block in range(C // 8):
        rows = slice(block * 8, block * 8 + 8)
        result = inverse_transform([(back[u, 0, rows], back[u, 1, rows]) for u in range(U)], middle[rows])
        for m in range(T):
            states[m, rows] = result[m]
    for m in range(1, T):
        tt = lax.rem(t + m, T)
        send(states.at[tt], out_ref.at[chunk(t)], s4.at[m], r4.at[m], tt, s)
    out_ref[chunk(t)] = states[pl.ds(t, 1)][0]
    for finish in sent:
        finish()
    for m in range(1, T):
        arrived(out_ref.at[chunk(lax.rem(t + T - m, T))], r4.at[m])


def body(forcing, initial, coupling, velocity):
    local_steps, zl, NY, NX = forcing.shape
    T = lax.axis_size("tm")
    S = lax.axis_size("space")
    U = T // 2
    NZ = zl * S
    C = zl * NY // T
    bands = 2 * S
    R = NY // bands
    RH = R + 2 * HALO
    WC = C + 2 * HALO
    q = C // R
    PK = RH + 3 * HALO
    PS = RH + HALO
    PF = R + HALO
    rows = R + 2 * GUARD
    reach = -(-GUARD // R)
    assert local_steps == 1 and SWEEPS == HALO <= R and ITERS == 2
    assert S % q == 0 and zl % 2 == 0 and T % 4 == 0
    assert C % R == 0 and NY % C == 0 and U * q == NZ and NZ % 8 == 0
    assert T & (T - 1) == 0 and S & (S - 1) == 0 and NZ & (NZ - 1) == 0
    assert (R * NZ // U) % 8 == 0 and (HALO * U) % R == 0 and WC <= NY
    f32 = jnp.float32
    dma = pltpu.SemaphoreType.DMA
    hbm = pl.BlockSpec(memory_space=pltpu.HBM)
    out = pl.pallas_call(
        lambda *refs: kernel((T, S, NY, NX, zl), *refs),
        out_shape=jax.ShapeDtypeStruct((zl * NY, NX), f32),
        in_specs=[hbm] * 4,
        out_specs=pl.BlockSpec(memory_space=pltpu.VMEM),
        scratch_shapes=[
            pltpu.VMEM((zl * NY, NX), f32),
            pltpu.VMEM((zl, WC + 2 * HALO, NX), f32),
            pltpu.VMEM((4, C, NX), f32),
            pltpu.VMEM((T, C, NX), f32),
            pltpu.VMEM((U, 2, C, NX), f32),
            pltpu.VMEM((2, C, NX), f32),
            pltpu.VMEM((4, NZ, PK, NX), f32),
            pltpu.VMEM((6, rows * NZ, NX), f32),
            pltpu.VMEM((3, rows * NZ, NX), f32),
            pltpu.VMEM((2, NZ * PS, NX), f32),
            pltpu.VMEM((2, rows * NZ, NX), f32),
            pltpu.VMEM((2, rows * NZ, NX), f32),
            pltpu.VMEM((2, rows * NZ, NX), f32),
            pltpu.VMEM((2, rows * NZ, NX), f32),
            pltpu.VMEM((R * NZ, NX), f32),
            pltpu.VMEM((U, R * NZ // U, NX), f32),
            pltpu.VMEM((R * NZ // U, NX), f32),
            pltpu.VMEM((RH * NZ, NX), f32),
            pltpu.VMEM((2, NZ * PF, NX), f32),
            pltpu.VMEM((U, 2, C, NX), f32),
            pltpu.VMEM((T, C, NX), f32),
            dma((6,)),
            dma((T,)),
            dma((T,)),
            dma((NZ, 3)),
            dma((NZ, 3)),
            dma((S, 2)),
            dma((S, 2)),
            dma((S, 2)),
            dma((S, 2)),
            dma((2,)),
            dma((2,)),
            dma((reach, 2)),
            dma((reach, 2)),
            dma((U,)),
            dma((U,)),
            dma((U, 3)),
            dma((U, 3)),
            dma((NZ,)),
            dma((U, q)),
            dma((T,)),
            dma((T,)),
        ],
        compiler_params=pltpu.CompilerParams(
            has_side_effects=True, collective_id=0, vmem_limit_bytes=48 * 1024 * 1024
        ),
    )(*[pltpu.with_memory_space_constraint(a, pltpu.HBM) for a in (forcing.reshape(zl * NY, NX), initial, coupling, velocity)])
    return out.reshape(forcing.shape)


def solution(mesh):
    return jax.shard_map(
        body,
        mesh=mesh,
        in_specs=(
            P("tm", "space", None, None),
            P("space", None, None),
            P("space", None, None),
            P(None, "space", None, None),
        ),
        out_specs=P("tm", "space", None, None),
        check_vma=False,
    )
```
